32 devices in a mesh: lat: 4 (over y, x), lon: 8 (over z, core).
Axes of the slice: x: 2, y: 2, z: 4, core: 2. Of those that a mesh axis runs over, the one named last changes fastest.
Arguments:
- transport: bfloat16 [48, 512, 3072], P(None, 'lat', 'lon'), may hold values from -0.0625 to 0.0625
- sigma_class: int32 [48, 512, 3072], P(None, 'lat', 'lon'), may hold values from 0 to 199
- basin_id: int32 [512, 3072], P('lat', 'lon'), may hold values from 0 to 3
- depth_levels: int32 [512, 3072], P('lat', 'lon'), may hold values from 0 to 48
Outputs:
- overturning: bfloat16 [4, 200, 512], replicated
The draws below stay inside these ranges and needn't reach their ends.
Inputs may be any that keep to these rules, and one draw needn't show every extreme that they name: `depth_levels`: 0 marks a land column.
All inputs are finite; a program needn't handle non-finite values.
Results may differ from the reference program's by a relative error of at most 0.001.
Values may be sent and summed in bfloat16 or wider, within the bound.
A program may use at most 64 MiB of HBM per device.

```python
import jax
import jax.numpy as jnp
from jax import lax

CLASSES = 200
BASINS = 4
ROWS_DEV = 128
COLS_DEV = 384
LEVELS = 48
NJ = 512
NI = 3072
N_LON = 8


def touch_ends(values, own_key, low, high):
    longest = values.shape.index(max(values.shape))
    spots = []
    for shift in (0, 1):
        where = [jax.random.randint(jax.random.fold_in(own_key, axis), (), 0, length) for axis, length in enumerate(values.shape)]
        where[longest] = (where[longest] + shift) % values.shape[longest]
        spots.append(tuple(where))
    return values.at[spots[0]].set(low).at[spots[1]].set(high)


def steps_of(key, dims, cuts, low, largest):
    def one(dim, shards_of):
        draws = jax.random.uniform(jax.random.fold_in(jax.random.fold_in(key, 6), dim), (shards_of,), jnp.float32, low / len(cuts), largest / len(cuts))
        return jnp.repeat(jnp.exp(draws), dims[dim] // shards_of).reshape((-1,) + (1,) * (len(dims) - dim - 1))

    factor_of = one(*cuts[0])
    for cut in cuts[1:]:
        factor_of = factor_of * one(*cut)
    return factor_of


def bell_draw(key, extent, deviation, reach, split=(), held_as=jnp.bfloat16):
    result = jax.random.normal(key, extent, jnp.float32) * deviation
    if len(split) > 0:
        result = steps_of(key, extent, split, -0.22, 0.18) * result
    return jnp.clip(result, min=-reach, max=reach).astype(held_as)


def setup_inputs(seed: int = 0) -> dict:
    key_of = jax.random.split(jax.random.key(seed), 5)
    return {
        "transport": bell_draw(key_of[0], (LEVELS, NJ, NI), (2.0 / (COLS_DEV * N_LON * LEVELS / BASINS) ** 0.5), 0.0625, ((1, 4), (2, 8))),
        "sigma_class": touch_ends(jax.random.randint(key_of[1], (LEVELS, NJ, NI), 0, CLASSES), jax.random.fold_in(key_of[1], 1), 0, CLASSES - 1).astype(jnp.int32),
        "basin_id": touch_ends(jax.random.randint(key_of[2], (NJ, NI), 0, BASINS), jax.random.fold_in(key_of[2], 1), 0, BASINS - 1).astype(jnp.int32),
        "depth_levels": touch_ends(jax.random.randint(key_of[3], (NJ, NI), 0, LEVELS + 1), jax.random.fold_in(key_of[3], 1), 0, LEVELS).astype(jnp.int32),
    }


def bin_block(transport, sigma_class, basin_id, depth_levels):
    depth_count, row_count, col_count = sigma_class.shape
    level_index = lax.broadcasted_iota(jnp.int32, (depth_count, row_count, col_count), 0)
    row_index = lax.broadcasted_iota(jnp.int32, (depth_count, row_count, col_count), 1)
    wet_cells = level_index < depth_levels[None, :, :]
    weights = jnp.where(wet_cells, transport.astype(jnp.float32), jnp.float32(0.0))
    bin_index = ((basin_id[None, :, :] * CLASSES + sigma_class) * row_count + row_index).astype(jnp.int32)
    flat = jax.ops.segment_sum(weights.reshape(-1), bin_index.reshape(-1), num_segments=BASINS * CLASSES * row_count)
    return flat.reshape(BASINS, CLASSES, row_count)


def reference(transport, sigma_class, basin_id, depth_levels):
    block_count = NJ // ROWS_DEV

    def one_block(start):
        return bin_block(
            lax.dynamic_slice_in_dim(transport, start, ROWS_DEV, 1),
            lax.dynamic_slice_in_dim(sigma_class, start, ROWS_DEV, 1),
            lax.dynamic_slice_in_dim(basin_id, start, ROWS_DEV, 0),
            lax.dynamic_slice_in_dim(depth_levels, start, ROWS_DEV, 0),
        )

    starts = (jnp.arange(block_count) * ROWS_DEV).astype(jnp.int32)
    tables = lax.map(one_block, starts)
    table = jnp.transpose(tables, (1, 2, 0, 3)).reshape(BASINS, CLASSES, NJ)
    return jnp.cumsum(table, axis=1).astype(jnp.bfloat16)
```

```python
import functools

import jax
import jax.numpy as jnp
import numpy as np
from jax import lax
from jax.experimental import pallas as pl
from jax.experimental.pallas import tpu as pltpu
from jax.sharding import PartitionSpec as P

CLASSES = 200
BASINS = 4
SUB = 8
LANES = 128
TILE = 256
STEP_ROWS = 16
MESH = pl.DeviceIdType.MESH
HIGHS = 26
HIGH_BLOCKS = 4
ONE_HOT = jnp.float8_e4m3fn


def high_rows(high, value):
    pair = jnp.concatenate([high, high - 1], axis=0).astype(jnp.int16)
    zero = jnp.bfloat16(0)
    return jnp.concatenate([jnp.where(pair == jnp.int16(i), value, zero) for i in range(0, HIGHS, 2)], axis=0)


def low_rows(low):
    four = jnp.concatenate([low - i for i in range(4)], axis=0).astype(jnp.int8)
    one, zero = ONE_HOT(1), ONE_HOT(0)
    return jnp.concatenate([jnp.where(four == jnp.int8(i), one, zero) for i in range(0, TILE // SUB, 4)], axis=0)


def squeeze_rows(product):
    rows = lax.broadcasted_iota(jnp.int32, (SUB, TILE), 0)
    lanes = lax.broadcasted_iota(jnp.int32, (SUB, TILE), 1)
    own = (lanes % SUB) == rows
    blocks = []
    for q in range(HIGH_BLOCKS):
        total = None
        for s in range(SUB):
            high = q * SUB + s
            if high * SUB >= CLASSES:
                break
            piece = jnp.where(own, product[high * SUB:(high + 1) * SUB, :], 0.0)
            piece = piece if s == 0 else pltpu.roll(piece, s, 1)
            total = piece if total is None else total + piece
        straight = jnp.where(rows == 0, total, 0.0)
        for r in range(1, SUB):
            straight = jnp.where(rows == r, pltpu.roll(total, TILE - r, 1), straight)
        blocks.append(straight)
    return jnp.concatenate(blocks, axis=1)


def bin_block(flow_ref, class_ref, basin_ref, depth_ref, out_ref, *accs):
    levels, _, cols = class_ref.shape
    chunks = cols // LANES
    per_trip = 24
    for half in range(STEP_ROWS // SUB):
        rows = slice(half * SUB, (half + 1) * SUB)

        def trip(t, carry, rows=rows):
            tiles = []
            for u in range(per_trip):
                level = t * per_trip + u
                for c in range(chunks):
                    lanes = slice(c * LANES, (c + 1) * LANES)
                    klass = class_ref[level, rows, lanes]
                    flow = flow_ref[level, :, lanes].astype(jnp.float32)[rows]
                    flow = jnp.where(level < depth_ref[rows, lanes], flow, 0.0)
                    value = jnp.concatenate([flow, flow], axis=0).astype(jnp.bfloat16)
                    low = basin_ref[rows, lanes] * SUB + (klass & 7)
                    tiles.append((high_rows(klass >> 3, value), low_rows(low)))
            for k in range(0, len(tiles), 2):
                mxu, stage = (k // 2) % 2, (k // 4) % 2
                left = jnp.concatenate([tiles[k][0], tiles[k + 1][0]], axis=1)
                right = jnp.concatenate([tiles[k][1], tiles[k + 1][1]], axis=1)
                pltpu.matmul_push_rhs(right, staging_register=stage, mxu_index=mxu, transpose=True)
                pltpu.matmul_acc_lhs(accs[mxu], left, load_staged_rhs=stage)
            return carry

        lax.fori_loop(0, levels // per_trip, trip, 0)
        product = pltpu.matmul_pop(accs[0]) + pltpu.matmul_pop(accs[1])
        out_ref[rows, :] = squeeze_rows(product)


def bin_kernel(*refs):
    shape = (HIGHS * SUB, TILE)
    pl.run_scoped(
        functools.partial(bin_block, *refs), *[pltpu.ACC(m)(shape, jnp.float32) for m in (0, 1)]
    )


def bin_rows(transport, sigma_class, basin_id, depth_levels):
    levels, row_count, cols = sigma_class.shape
    deep = pl.BlockSpec((levels, STEP_ROWS, cols), lambda i: (0, i, 0))
    flat = pl.BlockSpec((STEP_ROWS, cols), lambda i: (i, 0))
    width = HIGH_BLOCKS * TILE
    return pl.pallas_call(
        bin_kernel,
        grid=(row_count // STEP_ROWS,),
        in_specs=[deep, deep, flat, flat],
        out_specs=pl.BlockSpec((STEP_ROWS, width), lambda i: (i, 0)),
        out_shape=jax.ShapeDtypeStruct((row_count, width), jnp.float32),
        name="bin_rows",
    )(transport, sigma_class, basin_id, depth_levels)


def running_sums():
    row = np.arange(HIGH_BLOCKS * LANES)
    column = np.arange(2 * TILE)
    lane = row % LANES
    klass = (row // LANES) * 64 + (lane % SUB) * SUB + (lane % 64) // SUB
    same = (lane // 64)[:, None] == (column // TILE)[None, :]
    return (same & (klass[:, None] <= (column % TILE)[None, :])).astype(ONE_HOT)


def accumulate(share, sums, acc0, acc1):
    parts = []
    for pair in range(BASINS // 2):
        lanes = [share[:, q * TILE + pair * LANES:q * TILE + (pair + 1) * LANES] for q in range(HIGH_BLOCKS)]
        rest = jnp.concatenate(lanes, axis=1)
        for _ in range(3):
            part = rest.astype(jnp.bfloat16).astype(jnp.float32)
            rest = rest - part
            parts.append(part)
    left = jnp.concatenate(parts, axis=0).astype(jnp.bfloat16)
    rows = share.shape[0]
    for k in range(2):
        for n, acc in enumerate((acc0, acc1)):
            right = sums[k * TILE:(k + 1) * TILE, n * TILE:(n + 1) * TILE]
            pltpu.matmul_push_rhs(right, staging_register=k, mxu_index=n)
            pltpu.matmul_acc_lhs(acc, left[:, k * TILE:(k + 1) * TILE], load_staged_rhs=k)
    pieces = []
    halves = [pltpu.matmul_pop(acc0), pltpu.matmul_pop(acc1)]
    for pair in range(BASINS // 2):
        for total in halves:
            three = [total[(pair * 3 + i) * rows:(pair * 3 + i + 1) * rows] for i in range(3)]
            pieces.append(three[0] + three[1] + three[2])
    return jnp.concatenate(pieces, axis=1)


def share_kernel(lats, lons, table_ref, sums_ref, final_ref, out_ref, half, acc, arrived, sums, sum_sem,
                 half_send, half_recv, arr_send, arr_recv, out_send, out_recv):
    lat, lon = lax.axis_index("lat"), lax.axis_index("lon")
    zs = lons // 2
    z, core = lon // 2, lax.rem(lon, 2)
    partner = (lat, z * 2 + (1 - core))
    z_peers = [(lat, lax.rem(z + k, zs) * 2 + core) for k in range(1, zs)]
    lat_peers = [(lax.rem(lat + k, lats), lon) for k in range(1, lats)]

    load = pltpu.make_async_copy(sums_ref, sums, sum_sem)
    load.start()
    barrier = pltpu.get_barrier_semaphore()
    everyone = [partner] + z_peers + lat_peers
    for peer in everyone:
        pl.semaphore_signal(barrier, inc=1, device_id=peer, device_id_type=MESH)
    pl.semaphore_wait(barrier, len(everyone))

    def send(src, dst, send_sem, recv_sem, peer):
        copy = pltpu.make_async_remote_copy(
            src_ref=src, dst_ref=dst, send_sem=send_sem, recv_sem=recv_sem,
            device_id=peer, device_id_type=MESH,
        )
        copy.start()
        return copy

    swaps = []
    for k in [*range(1, zs), 0]:
        d = lax.rem(z + k, zs)
        swaps.append((k, send(table_ref.at[2 * d + (1 - core)], half.at[k], half_send.at[k], half_recv.at[k], partner)))
    moves = []
    for k, swap in swaps:
        swap.wait_recv()
        d = lax.rem(z + k, zs)
        acc[k] = table_ref[2 * d + core] + half[k]
        if k > 0:
            moves.append(send(acc.at[k], arrived.at[k - 1], arr_send.at[k - 1], arr_recv.at[k - 1], z_peers[k - 1]))
    share = acc[0]
    for k in range(1, zs):
        moves[k - 1].wait_recv()
        share = share + arrived[k - 1]
    load.wait()
    me = lat * lons + lon

    def cumulative(acc0, acc1):
        out_ref[me] = accumulate(share, sums[...], acc0, acc1).astype(jnp.bfloat16)

    shape = (6 * share.shape[0], TILE)
    pl.run_scoped(cumulative, *[pltpu.ACC(m)(shape, jnp.float32) for m in (0, 1)])

    copies = []

    def spread(owner, peer):
        n = len(copies)
        copies.append(send(out_ref.at[owner], out_ref.at[owner], out_send.at[n], out_recv.at[owner], peer))

    def landed(owner):
        pltpu.make_async_remote_copy(
            src_ref=out_ref.at[owner], dst_ref=out_ref.at[owner], send_sem=out_send.at[0],
            recv_sem=out_recv.at[owner], device_id=partner, device_id_type=MESH,
        ).wait_recv()

    for peer in z_peers + lat_peers:
        spread(me, peer)
    spread(me, partner)
    for k in range(1, zs):
        owner = lat * lons + lax.rem(z - k + zs, zs) * 2 + core
        landed(owner)
        for peer in lat_peers + [partner]:
            spread(owner, peer)
    for j in range(zs):
        for k in range(1, lats):
            owner = lax.rem(lat - k + lats, lats) * lons + lax.rem(z - j + zs, zs) * 2 + core
            landed(owner)
            spread(owner, partner)
    for j in range(zs):
        for k in range(lats):
            landed(lax.rem(lat - k + lats, lats) * lons + lax.rem(z - j + zs, zs) * 2 + (1 - core))
    rows = lons * share.shape[0]
    for group in range(lats):
        for basin in range(BASINS):
            block = out_ref[group * lons:(group + 1) * lons, :, basin * TILE:(basin + 1) * TILE]
            turned = jnp.transpose(block.reshape(rows, TILE))
            final_ref[basin, :, group * rows:(group + 1) * rows] = turned[:CLASSES]
    for _, swap in swaps:
        swap.wait_send()
    for move in moves:
        move.wait_send()
    for copy in copies:
        copy.wait_send()


def share_rows(lats, lons, table):
    rows = table.shape[0] // lons
    width = table.shape[1]
    zs = lons // 2
    sends = (zs - 1) + (lats - 1) + 1 + (zs - 1) * lats + zs * (lats - 1)
    dma = pltpu.SemaphoreType.DMA
    return pl.pallas_call(
        functools.partial(share_kernel, lats, lons),
        out_shape=jax.ShapeDtypeStruct((BASINS, CLASSES, lats * lons * rows), jnp.bfloat16),
        in_specs=[pl.BlockSpec(memory_space=pltpu.VMEM), pl.BlockSpec(memory_space=pl.ANY)],
        out_specs=pl.BlockSpec(memory_space=pltpu.VMEM),
        scratch_shapes=[
            pltpu.VMEM((lats * lons, rows, width), jnp.bfloat16),
            pltpu.VMEM((zs, rows, width), jnp.float32),
            pltpu.VMEM((zs, rows, width), jnp.float32),
            pltpu.VMEM((zs - 1, rows, width), jnp.float32),
            pltpu.VMEM((HIGH_BLOCKS * LANES, 2 * TILE), ONE_HOT),
            dma(()),
            dma((zs,)), dma((zs,)), dma((zs - 1,)), dma((zs - 1,)),
            dma((sends,)), dma((lats * lons,)),
        ],
        compiler_params=pltpu.CompilerParams(collective_id=0, has_side_effects=True),
        name="share_rows",
    )(table.reshape(lons, rows, width), jnp.asarray(running_sums()))


def body(lats, lons, transport, sigma_class, basin_id, depth_levels):
    table = bin_rows(transport, sigma_class, basin_id, depth_levels)
    return share_rows(lats, lons, table)


def solution(mesh):
    placed = (P(None, "lat", "lon"), P(None, "lat", "lon"), P("lat", "lon"), P("lat", "lon"))
    local = functools.partial(body, mesh.shape["lat"], mesh.shape["lon"])
    return jax.shard_map(local, mesh=mesh, in_specs=placed, out_specs=P(), check_vma=False)
```

```python
import functools

import jax
import jax.numpy as jnp
import numpy as np
from jax import lax
from jax.experimental import pallas as pl
from jax.experimental.pallas import tpu as pltpu
from jax.sharding import PartitionSpec as P

CLASSES = 200
BASINS = 4
SUB = 8
LANES = 128
TILE = 256
UNIT = 16
MESH = pl.DeviceIdType.MESH
HIGHS = 26
HIGH_BLOCKS = 4
ONE_HOT = jnp.float8_e4m3fn


def high_rows(high, value):
    pair = jnp.concatenate([high, high - 1], axis=0).astype(jnp.int16)
    zero = jnp.bfloat16(0)
    return jnp.concatenate([jnp.where(pair == jnp.int16(i), value, zero) for i in range(0, HIGHS, 2)], axis=0)


def low_rows(low):
    four = jnp.concatenate([low - i for i in range(4)], axis=0).astype(jnp.int8)
    one, zero = ONE_HOT(1), ONE_HOT(0)
    return jnp.concatenate([jnp.where(four == jnp.int8(i), one, zero) for i in range(0, TILE // SUB, 4)], axis=0)


def squeeze_rows(product):
    rows = lax.broadcasted_iota(jnp.int32, (SUB, TILE), 0)
    lanes = lax.broadcasted_iota(jnp.int32, (SUB, TILE), 1)
    own = (lanes % SUB) == rows
    blocks = []
    for q in range(HIGH_BLOCKS):
        total = None
        for s in range(SUB):
            high = q * SUB + s
            if high * SUB >= CLASSES:
                break
            piece = jnp.where(own, product[high * SUB:(high + 1) * SUB, :], 0.0)
            piece = piece if s == 0 else pltpu.roll(piece, s, 1)
            total = piece if total is None else total + piece
        straight = jnp.where(rows == 0, total, 0.0)
        for r in range(1, SUB):
            straight = jnp.where(rows == r, pltpu.roll(total, TILE - r, 1), straight)
        blocks.append(straight)
    return jnp.concatenate(blocks, axis=1)


def running_sums():
    row = np.arange(HIGH_BLOCKS * LANES)
    column = np.arange(2 * TILE)
    lane = row % LANES
    klass = (row // LANES) * 64 + (lane % SUB) * SUB + (lane % 64) // SUB
    same = (lane // 64)[:, None] == (column // TILE)[None, :]
    return (same & (klass[:, None] <= (column % TILE)[None, :])).astype(ONE_HOT)


def accumulate(share, sums, acc0, acc1):
    parts = []
    for pair in range(BASINS // 2):
        lanes = [share[:, q * TILE + pair * LANES:q * TILE + (pair + 1) * LANES] for q in range(HIGH_BLOCKS)]
        rest = jnp.concatenate(lanes, axis=1)
        for _ in range(3):
            part = rest.astype(jnp.bfloat16).astype(jnp.float32)
            rest = rest - part
            parts.append(part)
    left = jnp.concatenate(parts, axis=0).astype(jnp.bfloat16)
    rows = share.shape[0]
    for k in range(2):
        for n, acc in enumerate((acc0, acc1)):
            right = sums[k * TILE:(k + 1) * TILE, n * TILE:(n + 1) * TILE]
            pltpu.matmul_push_rhs(right, staging_register=k, mxu_index=n)
            pltpu.matmul_acc_lhs(acc, left[:, k * TILE:(k + 1) * TILE], load_staged_rhs=k)
    pieces = []
    halves = [pltpu.matmul_pop(acc0), pltpu.matmul_pop(acc1)]
    for pair in range(BASINS // 2):
        for total in halves:
            three = [total[(pair * 3 + i) * rows:(pair * 3 + i + 1) * rows] for i in range(3)]
            pieces.append(three[0] + three[1] + three[2])
    return jnp.concatenate(pieces, axis=1)


def bin_half(flow_ref, class_ref, basin_ref, depth_ref, half, accs):
    levels, _, cols = class_ref.shape
    rows = slice(half * SUB, (half + 1) * SUB)
    depth = depth_ref[rows, :]
    base = basin_ref[rows, :] * SUB
    lefts, rights = [], []
    count = 0
    for level in range(levels):
        klass = class_ref[level, rows, :]
        flow = flow_ref[level].astype(jnp.float32)[rows]
        flow = jnp.where(level < depth, flow, 0.0)
        value = jnp.concatenate([flow, flow], axis=0).astype(jnp.bfloat16)
        left = high_rows(klass >> 3, value)
        right = low_rows(base + (klass & 7))
        for lane in range(0, cols, LANES):
            lefts.append(left[:, lane:lane + LANES])
            rights.append(right[:, lane:lane + LANES])
            if len(lefts) == 2:
                mxu, stage = count % 2, (count // 2) % 2
                count += 1
                pltpu.matmul_push_rhs(
                    jnp.concatenate(rights, axis=1), staging_register=stage, mxu_index=mxu, transpose=True)
                pltpu.matmul_acc_lhs(accs[mxu], jnp.concatenate(lefts, axis=1), load_staged_rhs=stage)
                lefts, rights = [], []


def drain(accs):
    return squeeze_rows(pltpu.matmul_pop(accs[0]) + pltpu.matmul_pop(accs[1]))


def fused_body(lats, lons, flow_ref, class_ref, basin_ref, depth_ref, sums_ref, out_ref,
               flows, classes, basins, depths, sums, table, half, acc, arrived, in_sems, misc_sems,
               half_send, half_recv, arr_send, arr_recv, out_send, own_send, fwd_send, out_recv,
               a0, a1, b0, b1, c0, c1):
    lat, lon = lax.axis_index("lat"), lax.axis_index("lon")
    zs = lons // 2
    z, core = lon // 2, lax.rem(lon, 2)
    units = classes.shape[0]
    partner = (lat, z * 2 + (1 - core))
    z_peers = [(lat, lax.rem(z + k, zs) * 2 + core) for k in range(1, zs)]
    lat_peers = [(lax.rem(lat + k, lats), lon) for k in range(1, lats)]

    def fetch(u):
        rows = pl.ds(pl.multiple_of(u * UNIT, UNIT), UNIT)
        return [
            pltpu.make_async_copy(flow_ref.at[:, rows, :], flows.at[u], in_sems.at[0, u]),
            pltpu.make_async_copy(class_ref.at[:, rows, :], classes.at[u], in_sems.at[1, u]),
            pltpu.make_async_copy(basin_ref.at[rows, :], basins.at[u], in_sems.at[2, u]),
            pltpu.make_async_copy(depth_ref.at[rows, :], depths.at[u], in_sems.at[3, u]),
        ]

    for u in range(units):
        for copy in fetch(u):
            copy.start()
    load = pltpu.make_async_copy(sums_ref, sums, misc_sems.at[0])
    load.start()
    barrier = pltpu.get_barrier_semaphore()
    everyone = [partner] + z_peers + lat_peers
    for peer in everyone:
        pl.semaphore_signal(barrier, inc=1, device_id=peer, device_id_type=MESH)
    pl.semaphore_wait(barrier, len(everyone))
    load.wait()

    def remote(src, dst, send_sem, recv_sem, peer):
        return pltpu.make_async_remote_copy(
            src_ref=src, dst_ref=dst, send_sem=send_sem, recv_sem=recv_sem,
            device_id=peer, device_id_type=MESH,
        )

    def owner_lon(u):
        return lax.rem(u + lons // 2, lons)

    def swap_copy(u):
        return remote(table.at[u + 1], half.at[u], half_send.at[u], half_recv.at[u], partner)

    def move_copy(u, k):
        return remote(acc.at[u], arrived.at[u, k - 1], arr_send.at[u], arr_recv.at[u, k - 1], z_peers[k - 1])

    def block_at(group, u):
        return out_ref.at[group * units + u]

    def block_copy(group, u, send_sem, peer):
        ref = block_at(group, u)
        return remote(ref, ref, send_sem, out_recv.at[group * units + u], peer)

    def landed(group, u):
        block_copy(group, u, own_send.at[0, 0], partner).wait_recv()

    def swap(u):
        @pl.when(lax.rem(owner_lon(u), 2) != core)
        def _():
            swap_copy(u).start()

    def merge(u):
        target = owner_lon(u)

        @pl.when(lax.rem(target, 2) == core)
        def _():
            swap_copy(u).wait_recv()
            acc[u] = table[u + 1].reshape(UNIT, -1) + half[u].reshape(UNIT, -1)
            for k in range(1, zs):
                @pl.when(target // 2 == lax.rem(z + k, zs))
                def _(k=k):
                    move_copy(u, k).start()

    def own_peers():
        return z_peers + lat_peers + [partner]

    def finish(u):
        @pl.when(owner_lon(u) == lon)
        def _():
            for k in range(1, zs):
                move_copy(u, k).wait_recv()
            share = acc[u]
            for k in range(1, zs):
                share = share + arrived[u, k - 1]
            out_ref[lat * units + u] = accumulate(share, sums[...], c0, c1).astype(jnp.bfloat16)
            for n, peer in enumerate(own_peers()):
                block_copy(lat, u, own_send.at[u, n], peer).start()

    def forward(u):
        target = owner_lon(u)

        @pl.when((lax.rem(target, 2) == core) & (target != lon))
        def _():
            landed(lat, u)
            for n, peer in enumerate(lat_peers + [partner]):
                block_copy(lat, u, own_send.at[u, n], peer).start()

    def relay(u):
        @pl.when(lax.rem(owner_lon(u), 2) == core)
        def _():
            for k in range(1, lats):
                group = lax.rem(lat - k + lats, lats)
                landed(group, u)
                block_copy(group, u, fwd_send.at[u, k - 1], partner).start()

    def when_unit(u, stage):
        @pl.when((u >= 0) & (u < units))
        def _():
            stage(u)

    def step(t, carry):
        for copy in fetch(t):
            copy.wait()
        refs = [flows.at[t], classes.at[t], basins.at[t], depths.at[t]]
        table[t, 1] = drain((b0, b1))
        bin_half(*refs, 0, (a0, a1))
        when_unit(t - 1, swap)
        table[t + 1, 0] = drain((a0, a1))
        bin_half(*refs, 1, (b0, b1))
        when_unit(t - 1, merge)
        when_unit(t - 2, finish)
        when_unit(t - 3, forward)
        when_unit(t - 4, relay)
        return carry

    lax.fori_loop(0, units, step, 0)
    table[units, 1] = drain((b0, b1))
    last = units - 1
    swap(last)
    for stage, u in ((finish, last - 1), (merge, last), (forward, last - 2), (relay, last - 3),
                     (finish, last), (forward, last - 1), (relay, last - 2), (forward, last),
                     (relay, last - 1), (relay, last)):
        if u >= 0:
            stage(u)

    def settle(u, carry):
        target = owner_lon(u)

        @pl.when(lax.rem(target, 2) != core)
        def _():
            swap_copy(u).wait_send()
            for group in range(lats):
                landed(group, u)

        @pl.when(lax.rem(target, 2) == core)
        def _():
            for k in range(1, lats):
                block_copy(lat, u, fwd_send.at[u, k - 1], partner).wait_send()

            @pl.when(target == lon)
            def _():
                for n, peer in enumerate(own_peers()):
                    block_copy(lat, u, own_send.at[u, n], peer).wait_send()

            @pl.when(target != lon)
            def _():
                move_copy(u, 1).wait_send()
                for n, peer in enumerate(lat_peers + [partner]):
                    block_copy(lat, u, own_send.at[u, n], peer).wait_send()
        return carry

    lax.fori_loop(0, units, settle, 0)


def fused_kernel(lats, lons, *refs):
    shape = (HIGHS * SUB, TILE)
    tail = (6 * UNIT, TILE)
    pl.run_scoped(
        functools.partial(fused_body, lats, lons, *refs),
        *[pltpu.ACC(m)(s, jnp.float32) for s in (shape, shape, tail) for m in (0, 1)],
    )


def fused(lats, lons, transport, sigma_class, basin_id, depth_levels):
    levels, row_count, cols = sigma_class.shape
    units = row_count // UNIT
    zs = lons // 2
    width = HIGH_BLOCKS * TILE
    dma = pltpu.SemaphoreType.DMA
    hbm = pl.BlockSpec(memory_space=pl.ANY)
    return pl.pallas_call(
        functools.partial(fused_kernel, lats, lons),
        out_shape=jax.ShapeDtypeStruct((lats * units, UNIT, width), jnp.bfloat16),
        in_specs=[hbm] * 5,
        out_specs=pl.BlockSpec(memory_space=pltpu.VMEM),
        scratch_shapes=[
            pltpu.VMEM((units, levels, UNIT, cols), jnp.bfloat16),
            pltpu.VMEM((units, levels, UNIT, cols), jnp.int32),
            pltpu.VMEM((units, UNIT, cols), jnp.int32),
            pltpu.VMEM((units, UNIT, cols), jnp.int32),
            pltpu.VMEM((HIGH_BLOCKS * LANES, 2 * TILE), ONE_HOT),
            pltpu.VMEM((units + 1, 2, SUB, width), jnp.float32),
            pltpu.VMEM((units, 2, SUB, width), jnp.float32),
            pltpu.VMEM((units, UNIT, width), jnp.float32),
            pltpu.VMEM((units, zs - 1, UNIT, width), jnp.float32),
            dma((4, units)), dma((1,)),
            dma((units,)), dma((units,)), dma((units,)), dma((units, zs - 1)),
            dma((1,)), dma((units, zs - 1 + lats)), dma((units, lats - 1)), dma((lats * units,)),
        ],
        compiler_params=pltpu.CompilerParams(collective_id=0, has_side_effects=True),
        name="fused_rows",
    )(transport, sigma_class, basin_id, depth_levels, jnp.asarray(running_sums()))


def turn_kernel(in_ref, out_ref):
    for basin in range(BASINS):
        block = in_ref[:, :, basin * TILE:(basin + 1) * TILE]
        turned = jnp.transpose(block.reshape(-1, TILE))
        out_ref[basin] = turned[:CLASSES]


def turn(whole):
    blocks, rows, width = whole.shape
    per = LANES // rows
    return pl.pallas_call(
        turn_kernel,
        grid=(blocks // per,),
        in_specs=[pl.BlockSpec((per, rows, width), lambda i: (i, 0, 0))],
        out_specs=pl.BlockSpec((BASINS, CLASSES, LANES), lambda i: (0, 0, i)),
        out_shape=jax.ShapeDtypeStruct((BASINS, CLASSES, blocks * rows), jnp.bfloat16),
        name="turn_rows",
    )(whole)


def body(lats, lons, transport, sigma_class, basin_id, depth_levels):
    return turn(fused(lats, lons, transport, sigma_class, basin_id, depth_levels))


def solution(mesh):
    placed = (P(None, "lat", "lon"), P(None, "lat", "lon"), P("lat", "lon"), P("lat", "lon"))
    local = functools.partial(body, mesh.shape["lat"], mesh.shape["lon"])
    return jax.shard_map(local, mesh=mesh, in_specs=placed, out_specs=P(), check_vma=False)
```

```python
import functools

import jax
import jax.numpy as jnp
import numpy as np
from jax import lax
from jax.experimental import pallas as pl
from jax.experimental.pallas import tpu as pltpu
from jax.sharding import PartitionSpec as P

CLASSES = 200
BASINS = 4
SUB = 8
LANES = 128
TILE = 256
UNIT = 16
MESH = pl.DeviceIdType.MESH
HIGHS = 26
HIGH_BLOCKS = 4
ONE_HOT = jnp.float8_e4m3fn


def high_rows(high, value):
    pair = jnp.concatenate([high, high - 1], axis=0).astype(jnp.int16)
    zero = jnp.bfloat16(0)
    return jnp.concatenate([jnp.where(pair == jnp.int16(i), value, zero) for i in range(0, HIGHS, 2)], axis=0)


def low_rows(low):
    four = jnp.concatenate([low - i for i in range(4)], axis=0).astype(jnp.int8)
    one, zero = ONE_HOT(1), ONE_HOT(0)
    return jnp.concatenate([jnp.where(four == jnp.int8(i), one, zero) for i in range(0, TILE // SUB, 4)], axis=0)


def squeeze_rows(product):
    rows = lax.broadcasted_iota(jnp.int32, (SUB, TILE), 0)
    lanes = lax.broadcasted_iota(jnp.int32, (SUB, TILE), 1)
    own = (lanes % SUB) == rows
    blocks = []
    for q in range(HIGH_BLOCKS):
        total = None
        for s in range(SUB):
            high = q * SUB + s
            if high * SUB >= CLASSES:
                break
            piece = jnp.where(own, product[high * SUB:(high + 1) * SUB, :], 0.0)
            piece = piece if s == 0 else pltpu.roll(piece, s, 1)
            total = piece if total is None else total + piece
        straight = jnp.where(rows == 0, total, 0.0)
        for r in range(1, SUB):
            straight = jnp.where(rows == r, pltpu.roll(total, TILE - r, 1), straight)
        blocks.append(straight)
    return jnp.concatenate(blocks, axis=1)


def running_sums():
    row = np.arange(HIGH_BLOCKS * LANES)
    column = np.arange(2 * TILE)
    lane = row % LANES
    klass = (row // LANES) * 64 + (lane % SUB) * SUB + (lane % 64) // SUB
    same = (lane // 64)[:, None] == (column // TILE)[None, :]
    return (same & (klass[:, None] <= (column % TILE)[None, :])).astype(ONE_HOT)


def accumulate(share, sums, acc0, acc1):
    parts = []
    for pair in range(BASINS // 2):
        lanes = [share[:, q * TILE + pair * LANES:q * TILE + (pair + 1) * LANES] for q in range(HIGH_BLOCKS)]
        rest = jnp.concatenate(lanes, axis=1)
        for _ in range(3):
            part = rest.astype(jnp.bfloat16).astype(jnp.float32)
            rest = rest - part
            parts.append(part)
    left = jnp.concatenate(parts, axis=0).astype(jnp.bfloat16)
    rows = share.shape[0]
    for k in range(2):
        for n, acc in enumerate((acc0, acc1)):
            right = sums[k * TILE:(k + 1) * TILE, n * TILE:(n + 1) * TILE]
            pltpu.matmul_push_rhs(right, staging_register=k, mxu_index=n)
            pltpu.matmul_acc_lhs(acc, left[:, k * TILE:(k + 1) * TILE], load_staged_rhs=k)
    pieces = []
    halves = [pltpu.matmul_pop(acc0), pltpu.matmul_pop(acc1)]
    for pair in range(BASINS // 2):
        for total in halves:
            three = [total[(pair * 3 + i) * rows:(pair * 3 + i + 1) * rows] for i in range(3)]
            pieces.append(three[0] + three[1] + three[2])
    return jnp.concatenate(pieces, axis=1)


def bin_half(flow_ref, class_ref, basin_ref, depth_ref, half, accs):
    levels, _, cols = class_ref.shape
    rows = slice(half * SUB, (half + 1) * SUB)
    depth = depth_ref[rows, :]
    base = basin_ref[rows, :] * SUB
    lefts, rights = [], []
    count = 0
    for level in range(levels):
        klass = class_ref[level, rows, :]
        flow = flow_ref[level].astype(jnp.float32)[rows]
        flow = jnp.where(level < depth, flow, 0.0)
        value = jnp.concatenate([flow, flow], axis=0).astype(jnp.bfloat16)
        left = high_rows(klass >> 3, value)
        right = low_rows(base + (klass & 7))
        for lane in range(0, cols, LANES):
            lefts.append(left[:, lane:lane + LANES])
            rights.append(right[:, lane:lane + LANES])
            if len(lefts) == 2:
                mxu, stage = count % 2, (count // 2) % 2
                count += 1
                pltpu.matmul_push_rhs(
                    jnp.concatenate(rights, axis=1), staging_register=stage, mxu_index=mxu, transpose=True)
                pltpu.matmul_acc_lhs(accs[mxu], jnp.concatenate(lefts, axis=1), load_staged_rhs=stage)
                lefts, rights = [], []


def drain(accs):
    return squeeze_rows(pltpu.matmul_pop(accs[0]) + pltpu.matmul_pop(accs[1]))


def fused_body(lats, lons, flow_ref, class_ref, basin_ref, depth_ref, sums_ref, out_ref,
               flows, classes, basins, depths, sums, table, half, acc, arrived, mine, in_sems, misc_sems,
               half_send, half_recv, arr_send, arr_recv, own_sem, own_send, fwd_send, out_recv,
               a0, a1, b0, b1, c0, c1):
    lat, lon = lax.axis_index("lat"), lax.axis_index("lon")
    zs = lons // 2
    z, core = lon // 2, lax.rem(lon, 2)
    units = classes.shape[0]
    partner = (lat, z * 2 + (1 - core))
    z_peers = [(lat, lax.rem(z + k, zs) * 2 + core) for k in range(1, zs)]
    lat_peers = [(lax.rem(lat + k, lats), lon) for k in range(1, lats)]

    def fetch(u):
        rows = pl.ds(pl.multiple_of(u * UNIT, UNIT), UNIT)
        return [
            pltpu.make_async_copy(flow_ref.at[:, rows, :], flows.at[u], in_sems.at[0, u]),
            pltpu.make_async_copy(class_ref.at[:, rows, :], classes.at[u], in_sems.at[1, u]),
            pltpu.make_async_copy(basin_ref.at[rows, :], basins.at[u], in_sems.at[2, u]),
            pltpu.make_async_copy(depth_ref.at[rows, :], depths.at[u], in_sems.at[3, u]),
        ]

    for u in range(units):
        for copy in fetch(u):
            copy.start()
    load = pltpu.make_async_copy(sums_ref, sums, misc_sems.at[0])
    load.start()
    barrier = pltpu.get_barrier_semaphore()
    everyone = [partner] + z_peers + lat_peers
    for peer in everyone:
        pl.semaphore_signal(barrier, inc=1, device_id=peer, device_id_type=MESH)
    pl.semaphore_wait(barrier, len(everyone))
    load.wait()

    def remote(src, dst, send_sem, recv_sem, peer):
        return pltpu.make_async_remote_copy(
            src_ref=src, dst_ref=dst, send_sem=send_sem, recv_sem=recv_sem,
            device_id=peer, device_id_type=MESH,
        )

    def owner_lon(u):
        return lax.rem(u + lons // 2, lons)

    def swap_copy(u):
        return remote(table.at[u + 1], half.at[u], half_send.at[u], half_recv.at[u], partner)

    def move_copy(u, k):
        return remote(acc.at[u], arrived.at[u, k - 1], arr_send.at[u], arr_recv.at[u, k - 1], z_peers[k - 1])

    def block_at(group, u):
        return out_ref.at[group * units + u]

    def block_copy(group, u, send_sem, peer):
        ref = block_at(group, u)
        return remote(ref, ref, send_sem, out_recv.at[group * units + u], peer)

    def own_copy(u, n, peer):
        return remote(mine.at[u], block_at(lat, u), own_send.at[u, n], out_recv.at[lat * units + u], peer)

    def keep_copy(u):
        return pltpu.make_async_copy(mine.at[u], block_at(lat, u), own_sem.at[u])

    def landed(group, u):
        block_copy(group, u, own_send.at[0, 0], partner).wait_recv()

    def swap(u):
        @pl.when(lax.rem(owner_lon(u), 2) != core)
        def _():
            swap_copy(u).start()

    def merge(u):
        target = owner_lon(u)

        @pl.when(lax.rem(target, 2) == core)
        def _():
            swap_copy(u).wait_recv()
            acc[u] = table[u + 1].reshape(UNIT, -1) + half[u].reshape(UNIT, -1)
            for k in range(1, zs):
                @pl.when(target // 2 == lax.rem(z + k, zs))
                def _(k=k):
                    move_copy(u, k).start()

    def own_peers():
        return z_peers + lat_peers + [partner]

    def finish(u):
        @pl.when(owner_lon(u) == lon)
        def _():
            for k in range(1, zs):
                move_copy(u, k).wait_recv()
            share = acc[u]
            for k in range(1, zs):
                share = share + arrived[u, k - 1]
            mine[u] = accumulate(share, sums[...], c0, c1).astype(jnp.bfloat16)
            for n, peer in enumerate(own_peers()):
                own_copy(u, n, peer).start()
            keep_copy(u).start()

    def forward(u):
        target = owner_lon(u)

        @pl.when((lax.rem(target, 2) == core) & (target != lon))
        def _():
            landed(lat, u)
            for n, peer in enumerate(lat_peers + [partner]):
                block_copy(lat, u, own_send.at[u, n], peer).start()

    def relay(u):
        @pl.when(lax.rem(owner_lon(u), 2) == core)
        def _():
            for k in range(1, lats):
                group = lax.rem(lat - k + lats, lats)
                landed(group, u)
                block_copy(group, u, fwd_send.at[u, k - 1], partner).start()

    def when_unit(u, stage):
        @pl.when((u >= 0) & (u < units))
        def _():
            stage(u)

    def step(t, carry):
        for copy in fetch(t):
            copy.wait()
        refs = [flows.at[t], classes.at[t], basins.at[t], depths.at[t]]
        table[t, 1] = drain((b0, b1))
        bin_half(*refs, 0, (a0, a1))
        when_unit(t - 1, swap)
        table[t + 1, 0] = drain((a0, a1))
        bin_half(*refs, 1, (b0, b1))
        when_unit(t - 1, merge)
        when_unit(t - 2, finish)
        when_unit(t - 3, forward)
        when_unit(t - 4, relay)
        return carry

    lax.fori_loop(0, units, step, 0)
    table[units, 1] = drain((b0, b1))
    last = units - 1
    swap(last)
    for stage, u in ((finish, last - 1), (merge, last), (forward, last - 2), (relay, last - 3),
                     (finish, last), (forward, last - 1), (relay, last - 2), (forward, last),
                     (relay, last - 1), (relay, last)):
        if u >= 0:
            stage(u)

    def settle(u, carry):
        target = owner_lon(u)

        @pl.when(lax.rem(target, 2) != core)
        def _():
            swap_copy(u).wait_send()
            for group in range(lats):
                landed(group, u)

        @pl.when(lax.rem(target, 2) == core)
        def _():
            for k in range(1, lats):
                block_copy(lat, u, fwd_send.at[u, k - 1], partner).wait_send()

            @pl.when(target == lon)
            def _():
                for n, peer in enumerate(own_peers()):
                    own_copy(u, n, peer).wait_send()
                keep_copy(u).wait()

            @pl.when(target != lon)
            def _():
                move_copy(u, 1).wait_send()
                for n, peer in enumerate(lat_peers + [partner]):
                    block_copy(lat, u, own_send.at[u, n], peer).wait_send()
        return carry

    lax.fori_loop(0, units, settle, 0)


def fused_kernel(lats, lons, *refs):
    shape = (HIGHS * SUB, TILE)
    tail = (6 * UNIT, TILE)
    pl.run_scoped(
        functools.partial(fused_body, lats, lons, *refs),
        *[pltpu.ACC(m)(s, jnp.float32) for s in (shape, shape, tail) for m in (0, 1)],
    )


def fused(lats, lons, transport, sigma_class, basin_id, depth_levels):
    levels, row_count, cols = sigma_class.shape
    units = row_count // UNIT
    zs = lons // 2
    width = HIGH_BLOCKS * TILE
    dma = pltpu.SemaphoreType.DMA
    hbm = pl.BlockSpec(memory_space=pltpu.HBM)
    operands = (transport, sigma_class, basin_id, depth_levels, jnp.asarray(running_sums()))
    return pl.pallas_call(
        functools.partial(fused_kernel, lats, lons),
        out_shape=jax.ShapeDtypeStruct((lats * units, UNIT, width), jnp.bfloat16),
        in_specs=[hbm] * 5,
        out_specs=pl.BlockSpec(memory_space=pl.ANY),
        scratch_shapes=[
            pltpu.VMEM((units, levels, UNIT, cols), jnp.bfloat16),
            pltpu.VMEM((units, levels, UNIT, cols), jnp.int32),
            pltpu.VMEM((units, UNIT, cols), jnp.int32),
            pltpu.VMEM((units, UNIT, cols), jnp.int32),
            pltpu.VMEM((HIGH_BLOCKS * LANES, 2 * TILE), ONE_HOT),
            pltpu.VMEM((units + 1, 2, SUB, width), jnp.float32),
            pltpu.VMEM((units, 2, SUB, width), jnp.float32),
            pltpu.VMEM((units, UNIT, width), jnp.float32),
            pltpu.VMEM((units, zs - 1, UNIT, width), jnp.float32),
            pltpu.VMEM((units, UNIT, width), jnp.bfloat16),
            dma((4, units)), dma((1,)),
            dma((units,)), dma((units,)), dma((units,)), dma((units, zs - 1)),
            dma((units,)), dma((units, zs - 1 + lats)), dma((units, lats - 1)), dma((lats * units,)),
        ],
        compiler_params=pltpu.CompilerParams(
            collective_id=0, has_side_effects=True, vmem_limit_bytes=40 * 1024 * 1024),
        name="fused_rows",
    )(*[pltpu.with_memory_space_constraint(x, pltpu.HBM) for x in operands])


def turn_kernel(in_ref, out_ref, turned, sems):
    blocks, rows, _ = in_ref.shape
    copies = []
    for basin in range(BASINS):
        for lane in range(0, blocks * rows, LANES):
            block = in_ref[lane // rows:(lane + LANES) // rows, :, basin * TILE:(basin + 1) * TILE]
            turned[basin, :, lane:lane + LANES] = jnp.transpose(block.reshape(LANES, TILE))[:CLASSES]
        copies.append(pltpu.make_async_copy(turned.at[basin], out_ref.at[basin], sems.at[basin]))
        copies[-1].start()
    for copy in copies:
        copy.wait()


def turn(whole):
    blocks, rows, width = whole.shape
    shape = (BASINS, CLASSES, blocks * rows)
    return pl.pallas_call(
        turn_kernel,
        in_specs=[pl.BlockSpec(memory_space=pltpu.VMEM)],
        out_specs=pl.BlockSpec(memory_space=pl.ANY),
        out_shape=jax.ShapeDtypeStruct(shape, jnp.bfloat16),
        scratch_shapes=[pltpu.VMEM(shape, jnp.bfloat16), pltpu.SemaphoreType.DMA((BASINS,))],
        compiler_params=pltpu.CompilerParams(vmem_limit_bytes=16 * 1024 * 1024),
        name="turn_rows",
    )(whole)


def body(lats, lons, transport, sigma_class, basin_id, depth_levels):
    return turn(fused(lats, lons, transport, sigma_class, basin_id, depth_levels))


def solution(mesh):
    placed = (P(None, "lat", "lon"), P(None, "lat", "lon"), P("lat", "lon"), P("lat", "lon"))
    local = functools.partial(body, mesh.shape["lat"], mesh.shape["lon"])
    return jax.shard_map(local, mesh=mesh, in_specs=placed, out_specs=P(), check_vma=False)
```

```python
import functools

import jax
import jax.numpy as jnp
import numpy as np
from jax import lax
from jax.experimental import pallas as pl
from jax.experimental.pallas import tpu as pltpu
from jax.sharding import PartitionSpec as P

CLASSES = 200
BASINS = 4
SUB = 8
LANES = 128
TILE = 256
UNIT = 16
MESH = pl.DeviceIdType.MESH
HIGHS = 26
HIGH_BLOCKS = 4
ONE_HOT = jnp.float8_e4m3fn


def high_rows(high, value):
    pair = jnp.concatenate([high, high - 1], axis=0).astype(jnp.int16)
    zero = jnp.bfloat16(0)
    return jnp.concatenate([jnp.where(pair == jnp.int16(i), value, zero) for i in range(0, HIGHS, 2)], axis=0)


def low_rows(low):
    four = jnp.concatenate([low - i for i in range(4)], axis=0).astype(jnp.int8)
    one, zero = ONE_HOT(1), ONE_HOT(0)
    return jnp.concatenate([jnp.where(four == jnp.int8(i), one, zero) for i in range(0, TILE // SUB, 4)], axis=0)


def squeeze_rows(product):
    rows = lax.broadcasted_iota(jnp.int32, (SUB, TILE), 0)
    lanes = lax.broadcasted_iota(jnp.int32, (SUB, TILE), 1)
    own = (lanes % SUB) == rows
    blocks = []
    for q in range(HIGH_BLOCKS):
        total = None
        for s in range(SUB):
            high = q * SUB + s
            if high * SUB >= CLASSES:
                break
            piece = jnp.where(own, product[high * SUB:(high + 1) * SUB, :], 0.0)
            piece = piece if s == 0 else pltpu.roll(piece, s, 1)
            total = piece if total is None else total + piece
        straight = jnp.where(rows == 0, total, 0.0)
        for r in range(1, SUB):
            straight = jnp.where(rows == r, pltpu.roll(total, TILE - r, 1), straight)
        blocks.append(straight)
    return jnp.concatenate(blocks, axis=1)


def running_sums():
    row = np.arange(HIGH_BLOCKS * LANES)
    column = np.arange(2 * TILE)
    lane = row % LANES
    klass = (row // LANES) * 64 + (lane % SUB) * SUB + (lane % 64) // SUB
    same = (lane // 64)[:, None] == (column // TILE)[None, :]
    return (same & (klass[:, None] <= (column % TILE)[None, :])).astype(ONE_HOT)


def accumulate(share, sums, acc0, acc1):
    parts = []
    for pair in range(BASINS // 2):
        lanes = [share[:, q * TILE + pair * LANES:q * TILE + (pair + 1) * LANES] for q in range(HIGH_BLOCKS)]
        rest = jnp.concatenate(lanes, axis=1)
        for _ in range(3):
            part = rest.astype(jnp.bfloat16).astype(jnp.float32)
            rest = rest - part
            parts.append(part)
    left = jnp.concatenate(parts, axis=0).astype(jnp.bfloat16)
    rows = share.shape[0]
    for k in range(2):
        for n, acc in enumerate((acc0, acc1)):
            right = sums[k * TILE:(k + 1) * TILE, n * TILE:(n + 1) * TILE]
            pltpu.matmul_push_rhs(right, staging_register=k, mxu_index=n)
            pltpu.matmul_acc_lhs(acc, left[:, k * TILE:(k + 1) * TILE], load_staged_rhs=k)
    pieces = []
    halves = [pltpu.matmul_pop(acc0), pltpu.matmul_pop(acc1)]
    for pair in range(BASINS // 2):
        for total in halves:
            three = [total[(pair * 3 + i) * rows:(pair * 3 + i + 1) * rows] for i in range(3)]
            pieces.append(three[0] + three[1] + three[2])
    return jnp.concatenate(pieces, axis=1)


def bin_half(flow_ref, class_ref, basin_ref, depth_ref, half, accs):
    levels, _, cols = class_ref.shape
    rows = slice(half * SUB, (half + 1) * SUB)
    depth = depth_ref[rows, :]
    base = basin_ref[rows, :] * SUB
    lefts, rights = [], []
    count = 0
    for level in range(levels):
        klass = class_ref[level, rows, :]
        flow = flow_ref[level].astype(jnp.float32)[rows]
        flow = jnp.where(level < depth, flow, 0.0)
        value = jnp.concatenate([flow, flow], axis=0).astype(jnp.bfloat16)
        left = high_rows(klass >> 3, value)
        right = low_rows(base + (klass & 7))
        for lane in range(0, cols, LANES):
            lefts.append(left[:, lane:lane + LANES])
            rights.append(right[:, lane:lane + LANES])
            if len(lefts) == 2:
                mxu, stage = count % 2, (count // 2) % 2
                count += 1
                pltpu.matmul_push_rhs(
                    jnp.concatenate(rights, axis=1), staging_register=stage, mxu_index=mxu, transpose=True)
                pltpu.matmul_acc_lhs(accs[mxu], jnp.concatenate(lefts, axis=1), load_staged_rhs=stage)
                lefts, rights = [], []


def drain(accs):
    return squeeze_rows(pltpu.matmul_pop(accs[0]) + pltpu.matmul_pop(accs[1]))


def fused_body(lats, lons, flow_ref, class_ref, basin_ref, depth_ref, sums_ref, out_ref,
               flows, classes, basins, depths, sums, table, arrived, mine, in_sems, sum_sem,
               move_send, move_recv, keep_sem, own_send, lat_send, out_recv, a0, a1, b0, b1, c0, c1):
    lat, lon = lax.axis_index("lat"), lax.axis_index("lon")
    steps = classes.shape[0]
    units = steps * (UNIT // SUB)
    column = [(lat, lax.rem(lon + k, lons)) for k in range(1, lons)]
    lat_peers = [(lax.rem(lat + k, lats), lon) for k in range(1, lats)]

    def fetch(t):
        rows = pl.ds(pl.multiple_of(t * UNIT, UNIT), UNIT)
        return [
            pltpu.make_async_copy(flow_ref.at[:, rows, :], flows.at[t], in_sems.at[0, t]),
            pltpu.make_async_copy(class_ref.at[:, rows, :], classes.at[t], in_sems.at[1, t]),
            pltpu.make_async_copy(basin_ref.at[rows, :], basins.at[t], in_sems.at[2, t]),
            pltpu.make_async_copy(depth_ref.at[rows, :], depths.at[t], in_sems.at[3, t]),
        ]

    for t in range(steps):
        for copy in fetch(t):
            copy.start()
    load = pltpu.make_async_copy(sums_ref, sums, sum_sem)
    load.start()
    barrier = pltpu.get_barrier_semaphore()
    for peer in column + lat_peers:
        pl.semaphore_signal(barrier, inc=1, device_id=peer, device_id_type=MESH)

    def remote(src, dst, send_sem, recv_sem, peer):
        return pltpu.make_async_remote_copy(
            src_ref=src, dst_ref=dst, send_sem=send_sem, recv_sem=recv_sem,
            device_id=peer, device_id_type=MESH,
        )

    def owner(u):
        return lax.rem(u + lons // 2, lons)

    def move_copy(u, k):
        return remote(table.at[u + 1], arrived.at[u, k - 1], move_send.at[u], move_recv.at[u, k - 1], (lat, owner(u)))

    def block_copy(group, u, n, peer):
        ref = out_ref.at[group * units + u]
        return remote(ref, ref, lat_send.at[u, n], out_recv.at[group * units + u], peer)

    def own_copy(u, send_sem, peer):
        return remote(mine.at[u], out_ref.at[lat * units + u], send_sem, out_recv.at[lat * units + u], peer)

    def keep_copy(u):
        return pltpu.make_async_copy(mine.at[u], out_ref.at[lat * units + u], keep_sem.at[u])

    def move(u):
        @pl.when(owner(u) != lon)
        def _():
            move_copy(u, lax.rem(lon - owner(u) + lons, lons)).start()

    def finish(u):
        @pl.when(owner(u) == lon)
        def _():
            for k in range(1, lons):
                move_copy(u, k).wait_recv()
            share = table[u + 1]
            for k in range(1, lons):
                share = share + arrived[u, k - 1]
            mine[u] = accumulate(share, sums[...], c0, c1).astype(jnp.bfloat16)
            for n, peer in enumerate(column):
                own_copy(u, own_send.at[u, n], peer).start()
            for n, peer in enumerate(lat_peers):
                own_copy(u, lat_send.at[u, n], peer).start()
            keep_copy(u).start()

    def forward(u):
        @pl.when(owner(u) != lon)
        def _():
            block_copy(lat, u, 0, column[0]).wait_recv()
            for n, peer in enumerate(lat_peers):
                block_copy(lat, u, n, peer).start()

    def slot(s):
        for stage, u in ((move, s - 1), (finish, s - 3), (forward, s - 5)):
            @pl.when(u >= 0)
            def _(stage=stage, u=u):
                stage(u)

    def step(t, carry):
        for copy in fetch(t):
            copy.wait()
        refs = [flows.at[t], classes.at[t], basins.at[t], depths.at[t]]
        table[2 * t] = drain((b0, b1))
        bin_half(*refs, 0, (a0, a1))

        @pl.when(t == 0)
        def _():
            pl.semaphore_wait(barrier, len(column) + len(lat_peers))
            load.wait()

        slot(2 * t)
        table[2 * t + 1] = drain((a0, a1))
        bin_half(*refs, 1, (b0, b1))
        slot(2 * t + 1)
        return carry

    lax.fori_loop(0, steps, step, 0)
    table[units] = drain((b0, b1))
    last = units - 1
    for stage, u in ((move, last), (finish, last - 2), (forward, last - 4), (finish, last - 1), (forward, last - 3),
                     (finish, last), (forward, last - 2), (forward, last - 1), (forward, last)):
        if u >= 0:
            stage(u)

    def settle(u, carry):
        for k in range(1, lats):
            block_copy(lax.rem(lat + k, lats), u, 0, column[0]).wait_recv()

        @pl.when(owner(u) == lon)
        def _():
            for n, peer in enumerate(column):
                own_copy(u, own_send.at[u, n], peer).wait_send()
            keep_copy(u).wait()

        @pl.when(owner(u) != lon)
        def _():
            move_copy(u, 1).wait_send()

        for n, peer in enumerate(lat_peers):
            block_copy(lat, u, n, peer).wait_send()
        return carry

    lax.fori_loop(0, units, settle, 0)


def fused_kernel(lats, lons, *refs):
    shape = (HIGHS * SUB, TILE)
    tail = (6 * SUB, TILE)
    pl.run_scoped(
        functools.partial(fused_body, lats, lons, *refs),
        *[pltpu.ACC(m)(s, jnp.float32) for s in (shape, shape, tail) for m in (0, 1)],
    )


def fused(lats, lons, transport, sigma_class, basin_id, depth_levels):
    levels, row_count, cols = sigma_class.shape
    steps = row_count // UNIT
    units = row_count // SUB
    width = HIGH_BLOCKS * TILE
    dma = pltpu.SemaphoreType.DMA
    hbm = pl.BlockSpec(memory_space=pltpu.HBM)
    operands = (transport, sigma_class, basin_id, depth_levels, jnp.asarray(running_sums()))
    return pl.pallas_call(
        functools.partial(fused_kernel, lats, lons),
        out_shape=jax.ShapeDtypeStruct((lats * units, SUB, width), jnp.bfloat16),
        in_specs=[hbm] * 5,
        out_specs=pl.BlockSpec(memory_space=pl.ANY),
        scratch_shapes=[
            pltpu.VMEM((steps, levels, UNIT, cols), jnp.bfloat16),
            pltpu.VMEM((steps, levels, UNIT, cols), jnp.int32),
            pltpu.VMEM((steps, UNIT, cols), jnp.int32),
            pltpu.VMEM((steps, UNIT, cols), jnp.int32),
            pltpu.VMEM((HIGH_BLOCKS * LANES, 2 * TILE), ONE_HOT),
            pltpu.VMEM((units + 1, SUB, width), jnp.float32),
            pltpu.VMEM((units, lons - 1, SUB, width), jnp.float32),
            pltpu.VMEM((units, SUB, width), jnp.bfloat16),
            dma((4, steps)), dma(()),
            dma((units,)), dma((units, lons - 1)), dma((units,)),
            dma((units, lons - 1)), dma((units, lats - 1)), dma((lats * units,)),
        ],
        compiler_params=pltpu.CompilerParams(
            collective_id=0, has_side_effects=True, vmem_limit_bytes=40 * 1024 * 1024),
        name="fused_rows",
    )(*[pltpu.with_memory_space_constraint(x, pltpu.HBM) for x in operands])


def turn_kernel(in_ref, out_ref, turned, sems):
    blocks, rows, _ = in_ref.shape
    copies = []
    for basin in range(BASINS):
        for lane in range(0, blocks * rows, LANES):
            block = in_ref[lane // rows:(lane + LANES) // rows, :, basin * TILE:(basin + 1) * TILE]
            turned[basin, :, lane:lane + LANES] = jnp.transpose(block.reshape(LANES, TILE))[:CLASSES]
        copies.append(pltpu.make_async_copy(turned.at[basin], out_ref.at[basin], sems.at[basin]))
        copies[-1].start()
    for copy in copies:
        copy.wait()


def turn(whole):
    blocks, rows, width = whole.shape
    shape = (BASINS, CLASSES, blocks * rows)
    return pl.pallas_call(
        turn_kernel,
        in_specs=[pl.BlockSpec(memory_space=pltpu.VMEM)],
        out_specs=pl.BlockSpec(memory_space=pl.ANY),
        out_shape=jax.ShapeDtypeStruct(shape, jnp.bfloat16),
        scratch_shapes=[pltpu.VMEM(shape, jnp.bfloat16), pltpu.SemaphoreType.DMA((BASINS,))],
        compiler_params=pltpu.CompilerParams(vmem_limit_bytes=16 * 1024 * 1024),
        name="turn_rows",
    )(whole)


def body(lats, lons, transport, sigma_class, basin_id, depth_levels):
    return turn(fused(lats, lons, transport, sigma_class, basin_id, depth_levels))


def solution(mesh):
    placed = (P(None, "lat", "lon"), P(None, "lat", "lon"), P("lat", "lon"), P("lat", "lon"))
    local = functools.partial(body, mesh.shape["lat"], mesh.shape["lon"])
    return jax.shard_map(local, mesh=mesh, in_specs=placed, out_specs=P(), check_vma=False)
```

```python
import functools

import jax
import jax.numpy as jnp
import numpy as np
from jax import lax
from jax.experimental import pallas as pl
from jax.experimental.pallas import tpu as pltpu
from jax.sharding import PartitionSpec as P

CLASSES = 200
BASINS = 4
SUB = 8
LANES = 128
TILE = 256
UNIT = 16
MESH = pl.DeviceIdType.MESH
HIGHS = 26
HIGH_BLOCKS = 4
ONE_HOT = jnp.float8_e4m3fn


def high_rows(high, value):
    pair = jnp.concatenate([high, high - 1], axis=0).astype(jnp.int16)
    zero = jnp.bfloat16(0)
    return jnp.concatenate([jnp.where(pair == jnp.int16(i), value, zero) for i in range(0, HIGHS, 2)], axis=0)


def low_rows(low):
    four = jnp.concatenate([low - i for i in range(4)], axis=0).astype(jnp.int8)
    one, zero = ONE_HOT(1), ONE_HOT(0)
    return jnp.concatenate([jnp.where(four == jnp.int8(i), one, zero) for i in range(0, TILE // SUB, 4)], axis=0)


def squeeze_rows(product):
    rows = lax.broadcasted_iota(jnp.int32, (SUB, TILE), 0)
    lanes = lax.broadcasted_iota(jnp.int32, (SUB, TILE), 1)
    own = (lanes % SUB) == rows
    blocks = []
    for q in range(HIGH_BLOCKS):
        total = None
        for s in range(SUB):
            high = q * SUB + s
            if high * SUB >= CLASSES:
                break
            piece = jnp.where(own, product[high * SUB:(high + 1) * SUB, :], 0.0)
            piece = piece if s == 0 else pltpu.roll(piece, s, 1)
            total = piece if total is None else total + piece
        straight = jnp.where(rows == 0, total, 0.0)
        for r in range(1, SUB):
            straight = jnp.where(rows == r, pltpu.roll(total, TILE - r, 1), straight)
        blocks.append(straight)
    return jnp.concatenate(blocks, axis=1)


def running_sums():
    row = np.arange(HIGH_BLOCKS * LANES)
    column = np.arange(2 * TILE)
    lane = row % LANES
    klass = (row // LANES) * 64 + (lane % SUB) * SUB + (lane % 64) // SUB
    same = (lane // 64)[:, None] == (column // TILE)[None, :]
    return (same & (klass[:, None] <= (column % TILE)[None, :])).astype(ONE_HOT)


def accumulate(share, sums, acc0, acc1):
    parts = []
    for pair in range(BASINS // 2):
        lanes = [share[:, q * TILE + pair * LANES:q * TILE + (pair + 1) * LANES] for q in range(HIGH_BLOCKS)]
        rest = jnp.concatenate(lanes, axis=1)
        for _ in range(3):
            part = rest.astype(jnp.bfloat16).astype(jnp.float32)
            rest = rest - part
            parts.append(part)
    left = jnp.concatenate(parts, axis=0).astype(jnp.bfloat16)
    rows = share.shape[0]
    for k in range(2):
        for n, acc in enumerate((acc0, acc1)):
            right = sums[k * TILE:(k + 1) * TILE, n * TILE:(n + 1) * TILE]
            pltpu.matmul_push_rhs(right, staging_register=k, mxu_index=n)
            pltpu.matmul_acc_lhs(acc, left[:, k * TILE:(k + 1) * TILE], load_staged_rhs=k)
    pieces = []
    halves = [pltpu.matmul_pop(acc0), pltpu.matmul_pop(acc1)]
    for pair in range(BASINS // 2):
        for total in halves:
            three = [total[(pair * 3 + i) * rows:(pair * 3 + i + 1) * rows] for i in range(3)]
            pieces.append(three[0] + three[1] + three[2])
    return jnp.concatenate(pieces, axis=1)


def bin_half(flow_ref, class_ref, basin_ref, depth_ref, half, accs):
    levels, _, cols = class_ref.shape
    rows = slice(half * SUB, (half + 1) * SUB)
    depth = depth_ref[rows, :]
    base = basin_ref[rows, :] * SUB
    lefts, rights = [], []
    count = 0
    for level in range(levels):
        klass = class_ref[level, rows, :]
        flow = flow_ref[level].astype(jnp.float32)[rows]
        flow = jnp.where(level < depth, flow, 0.0)
        value = jnp.concatenate([flow, flow], axis=0).astype(jnp.bfloat16)
        left = high_rows(klass >> 3, value)
        right = low_rows(base + (klass & 7))
        for lane in range(0, cols, LANES):
            lefts.append(left[:, lane:lane + LANES])
            rights.append(right[:, lane:lane + LANES])
            if len(lefts) == 2:
                mxu, stage = count % 2, (count // 2) % 2
                count += 1
                pltpu.matmul_push_rhs(
                    jnp.concatenate(rights, axis=1), staging_register=stage, mxu_index=mxu, transpose=True)
                pltpu.matmul_acc_lhs(accs[mxu], jnp.concatenate(lefts, axis=1), load_staged_rhs=stage)
                lefts, rights = [], []


def drain(accs):
    return squeeze_rows(pltpu.matmul_pop(accs[0]) + pltpu.matmul_pop(accs[1]))


def fused_body(lats, lons, flow_ref, class_ref, basin_ref, depth_ref, sums_ref, out_ref,
               flows, classes, basins, depths, sums, table, arrived, mine, in_sems, sum_sem,
               move_send, move_recv, keep_sem, own_send, lat_send, out_recv, a0, a1, b0, b1, c0, c1):
    lat, lon = lax.axis_index("lat"), lax.axis_index("lon")
    steps = classes.shape[0]
    units = steps * (UNIT // SUB)
    column = [(lat, lax.rem(lon + k, lons)) for k in range(1, lons)]
    lat_peers = [(lax.rem(lat + k, lats), lon) for k in range(1, lats)]

    def fetch(t):
        rows = pl.ds(pl.multiple_of(t * UNIT, UNIT), UNIT)
        return [
            pltpu.make_async_copy(flow_ref.at[:, rows, :], flows.at[t], in_sems.at[0, t]),
            pltpu.make_async_copy(class_ref.at[:, rows, :], classes.at[t], in_sems.at[1, t]),
            pltpu.make_async_copy(basin_ref.at[rows, :], basins.at[t], in_sems.at[2, t]),
            pltpu.make_async_copy(depth_ref.at[rows, :], depths.at[t], in_sems.at[3, t]),
        ]

    for t in range(steps):
        for copy in fetch(t):
            copy.start()
    load = pltpu.make_async_copy(sums_ref, sums, sum_sem)
    load.start()
    barrier = pltpu.get_barrier_semaphore()
    for peer in column + lat_peers:
        pl.semaphore_signal(barrier, inc=1, device_id=peer, device_id_type=MESH)

    def remote(src, dst, send_sem, recv_sem, peer):
        return pltpu.make_async_remote_copy(
            src_ref=src, dst_ref=dst, send_sem=send_sem, recv_sem=recv_sem,
            device_id=peer, device_id_type=MESH,
        )

    def owner(u):
        zs = lons // 2
        back = lax.rem(2 * units - 1 - u, lons)
        i = lax.rem(back, zs)
        z = zs // 2 - 1 - i // 2 + lax.rem(i, 2) * (1 + 2 * (i // 2))
        return 2 * z + lax.rem(1 + back + back // zs, 2)

    def move_copy(u, k):
        return remote(table.at[u + 1], arrived.at[u, k - 1], move_send.at[u], move_recv.at[u, k - 1], (lat, owner(u)))

    def block_copy(group, u, n, peer):
        ref = out_ref.at[group * units + u]
        return remote(ref, ref, lat_send.at[u, n], out_recv.at[group * units + u], peer)

    def own_copy(u, send_sem, peer):
        return remote(mine.at[u], out_ref.at[lat * units + u], send_sem, out_recv.at[lat * units + u], peer)

    def keep_copy(u):
        return pltpu.make_async_copy(mine.at[u], out_ref.at[lat * units + u], keep_sem.at[u])

    def move(u):
        @pl.when(owner(u) != lon)
        def _():
            move_copy(u, lax.rem(lon - owner(u) + lons, lons)).start()

    def finish(u):
        @pl.when(owner(u) == lon)
        def _():
            for k in range(1, lons):
                move_copy(u, k).wait_recv()
            share = table[u + 1]
            for k in range(1, lons):
                share = share + arrived[u, k - 1]
            mine[u] = accumulate(share, sums[...], c0, c1).astype(jnp.bfloat16)
            for n, peer in enumerate(column):
                own_copy(u, own_send.at[u, n], peer).start()
            for n, peer in enumerate(lat_peers):
                own_copy(u, lat_send.at[u, n], peer).start()
            keep_copy(u).start()

    def forward(u):
        @pl.when(owner(u) != lon)
        def _():
            block_copy(lat, u, 0, column[0]).wait_recv()
            for n, peer in enumerate(lat_peers):
                block_copy(lat, u, n, peer).start()

    def from_zero(stage, u):
        @pl.when(u >= 0)
        def _():
            stage(u)

    def bin_unit_pair(t, between):
        for copy in fetch(t):
            copy.wait()
        refs = [flows.at[t], classes.at[t], basins.at[t], depths.at[t]]
        table[2 * t] = drain((b0, b1))
        bin_half(*refs, 0, (a0, a1))
        between()
        table[2 * t + 1] = drain((a0, a1))
        bin_half(*refs, 1, (b0, b1))

    def step(t, carry):
        bin_unit_pair(t, lambda: move(2 * t - 1))
        move(2 * t)
        for stage, late in ((finish, 3), (finish, 2), (forward, 5), (forward, 4)):
            from_zero(stage, 2 * t - late)
        return carry

    bin_unit_pair(0, lambda: None)
    pl.semaphore_wait(barrier, len(column) + len(lat_peers))
    load.wait()
    move(0)
    lax.fori_loop(1, steps, step, 0)
    table[units] = drain((b0, b1))
    last = units - 1
    for stage, u in ((move, last), (finish, last - 2), (forward, last - 4), (finish, last - 1), (forward, last - 3),
                     (finish, last), (forward, last - 2), (forward, last - 1), (forward, last)):
        if u >= 0:
            stage(u)

    def settle(u, carry):
        for k in range(1, lats):
            block_copy(lax.rem(lat + k, lats), u, 0, column[0]).wait_recv()

        @pl.when(owner(u) == lon)
        def _():
            for n, peer in enumerate(column):
                own_copy(u, own_send.at[u, n], peer).wait_send()
            keep_copy(u).wait()

        @pl.when(owner(u) != lon)
        def _():
            move_copy(u, 1).wait_send()

        for n, peer in enumerate(lat_peers):
            block_copy(lat, u, n, peer).wait_send()
        return carry

    lax.fori_loop(0, units, settle, 0)


def fused_kernel(lats, lons, *refs):
    shape = (HIGHS * SUB, TILE)
    tail = (6 * SUB, TILE)
    pl.run_scoped(
        functools.partial(fused_body, lats, lons, *refs),
        *[pltpu.ACC(m)(s, jnp.float32) for s in (shape, shape, tail) for m in (0, 1)],
    )


def fused(lats, lons, transport, sigma_class, basin_id, depth_levels):
    levels, row_count, cols = sigma_class.shape
    steps = row_count // UNIT
    units = row_count // SUB
    width = HIGH_BLOCKS * TILE
    dma = pltpu.SemaphoreType.DMA
    hbm = pl.BlockSpec(memory_space=pltpu.HBM)
    operands = (transport, sigma_class, basin_id, depth_levels, jnp.asarray(running_sums()))
    return pl.pallas_call(
        functools.partial(fused_kernel, lats, lons),
        out_shape=jax.ShapeDtypeStruct((lats * units, SUB, width), jnp.bfloat16),
        in_specs=[hbm] * 5,
        out_specs=pl.BlockSpec(memory_space=pl.ANY),
        scratch_shapes=[
            pltpu.VMEM((steps, levels, UNIT, cols), jnp.bfloat16),
            pltpu.VMEM((steps, levels, UNIT, cols), jnp.int32),
            pltpu.VMEM((steps, UNIT, cols), jnp.int32),
            pltpu.VMEM((steps, UNIT, cols), jnp.int32),
            pltpu.VMEM((HIGH_BLOCKS * LANES, 2 * TILE), ONE_HOT),
            pltpu.VMEM((units + 1, SUB, width), jnp.float32),
            pltpu.VMEM((units, lons - 1, SUB, width), jnp.float32),
            pltpu.VMEM((units, SUB, width), jnp.bfloat16),
            dma((4, steps)), dma(()),
            dma((units,)), dma((units, lons - 1)), dma((units,)),
            dma((units, lons - 1)), dma((units, lats - 1)), dma((lats * units,)),
        ],
        compiler_params=pltpu.CompilerParams(
            collective_id=0, has_side_effects=True, vmem_limit_bytes=40 * 1024 * 1024),
        name="fused_rows",
    )(*[pltpu.with_memory_space_constraint(x, pltpu.HBM) for x in operands])


def turn_kernel(in_ref, out_ref, turned, sems):
    blocks, rows, _ = in_ref.shape
    copies = []
    for basin in range(BASINS):
        for lane in range(0, blocks * rows, LANES):
            block = in_ref[lane // rows:(lane + LANES) // rows, :, basin * TILE:(basin + 1) * TILE]
            turned[basin, :, lane:lane + LANES] = jnp.transpose(block.reshape(LANES, TILE))[:CLASSES]
        copies.append(pltpu.make_async_copy(turned.at[basin], out_ref.at[basin], sems.at[basin]))
        copies[-1].start()
    for copy in copies:
        copy.wait()


def turn(whole):
    blocks, rows, width = whole.shape
    shape = (BASINS, CLASSES, blocks * rows)
    return pl.pallas_call(
        turn_kernel,
        in_specs=[pl.BlockSpec(memory_space=pltpu.VMEM)],
        out_specs=pl.BlockSpec(memory_space=pl.ANY),
        out_shape=jax.ShapeDtypeStruct(shape, jnp.bfloat16),
        scratch_shapes=[pltpu.VMEM(shape, jnp.bfloat16), pltpu.SemaphoreType.DMA((BASINS,))],
        compiler_params=pltpu.CompilerParams(vmem_limit_bytes=16 * 1024 * 1024),
        name="turn_rows",
    )(whole)


def body(lats, lons, transport, sigma_class, basin_id, depth_levels):
    return turn(fused(lats, lons, transport, sigma_class, basin_id, depth_levels))


def solution(mesh):
    placed = (P(None, "lat", "lon"), P(None, "lat", "lon"), P("lat", "lon"), P("lat", "lon"))
    local = functools.partial(body, mesh.shape["lat"], mesh.shape["lon"])
    return jax.shard_map(local, mesh=mesh, in_specs=placed, out_specs=P(), check_vma=False)
```

```python
import functools

import jax
import jax.numpy as jnp
import numpy as np
from jax import lax
from jax.experimental import pallas as pl
from jax.experimental.pallas import tpu as pltpu
from jax.sharding import PartitionSpec as P

CLASSES = 200
BASINS = 4
SUB = 8
LANES = 128
TILE = 256
UNIT = 16
STEP = 32
MESH = pl.DeviceIdType.MESH
HIGHS = 26
HIGH_BLOCKS = 4
ONE_HOT = jnp.float8_e4m3fn


def high_rows(high, value):
    pair = jnp.concatenate([high, high - 1], axis=0).astype(jnp.int16)
    zero = jnp.bfloat16(0)
    return jnp.concatenate([jnp.where(pair == jnp.int16(i), value, zero) for i in range(0, HIGHS, 2)], axis=0)


def low_rows(low):
    four = jnp.concatenate([low - i for i in range(4)], axis=0).astype(jnp.int8)
    one, zero = ONE_HOT(1), ONE_HOT(0)
    return jnp.concatenate([jnp.where(four == jnp.int8(i), one, zero) for i in range(0, TILE // SUB, 4)], axis=0)


def squeeze_rows(product):
    rows = lax.broadcasted_iota(jnp.int32, (SUB, TILE), 0)
    lanes = lax.broadcasted_iota(jnp.int32, (SUB, TILE), 1)
    own = (lanes % SUB) == rows
    blocks = []
    for q in range(HIGH_BLOCKS):
        total = None
        for s in range(SUB):
            high = q * SUB + s
            if high * SUB >= CLASSES:
                break
            piece = jnp.where(own, product[high * SUB:(high + 1) * SUB, :], 0.0)
            piece = piece if s == 0 else pltpu.roll(piece, s, 1)
            total = piece if total is None else total + piece
        straight = jnp.where(rows == 0, total, 0.0)
        for r in range(1, SUB):
            straight = jnp.where(rows == r, pltpu.roll(total, TILE - r, 1), straight)
        blocks.append(straight)
    return jnp.concatenate(blocks, axis=1)


def running_sums():
    row = np.arange(HIGH_BLOCKS * LANES)
    column = np.arange(2 * TILE)
    lane = row % LANES
    klass = (row // LANES) * 64 + (lane % SUB) * SUB + (lane % 64) // SUB
    same = (lane // 64)[:, None] == (column // TILE)[None, :]
    return (same & (klass[:, None] <= (column % TILE)[None, :])).astype(ONE_HOT)


def accumulate(share, sums, acc0, acc1):
    parts = []
    for pair in range(BASINS // 2):
        lanes = [share[:, q * TILE + pair * LANES:q * TILE + (pair + 1) * LANES] for q in range(HIGH_BLOCKS)]
        rest = jnp.concatenate(lanes, axis=1)
        for _ in range(3):
            part = rest.astype(jnp.bfloat16).astype(jnp.float32)
            rest = rest - part
            parts.append(part)
    left = jnp.concatenate(parts, axis=0).astype(jnp.bfloat16)
    rows = share.shape[0]
    for k in range(2):
        for n, acc in enumerate((acc0, acc1)):
            right = sums[k * TILE:(k + 1) * TILE, n * TILE:(n + 1) * TILE]
            pltpu.matmul_push_rhs(right, staging_register=k, mxu_index=n)
            pltpu.matmul_acc_lhs(acc, left[:, k * TILE:(k + 1) * TILE], load_staged_rhs=k)
    pieces = []
    halves = [pltpu.matmul_pop(acc0), pltpu.matmul_pop(acc1)]
    for pair in range(BASINS // 2):
        for total in halves:
            three = [total[(pair * 3 + i) * rows:(pair * 3 + i + 1) * rows] for i in range(3)]
            pieces.append(three[0] + three[1] + three[2])
    return jnp.concatenate(pieces, axis=1)


def bin_half(flow_ref, class_ref, basin_ref, depth_ref, half, accs, middle=None):
    levels, _, cols = class_ref.shape
    rows = slice(half * SUB, (half + 1) * SUB)
    depth = depth_ref[rows, :]
    base = basin_ref[rows, :] * SUB
    lefts, rights = [], []
    count = 0
    for level in range(levels):
        if level == levels // 2 and middle is not None:
            middle()
        klass = class_ref[level, rows, :]
        flow = flow_ref[level].astype(jnp.float32)[rows]
        flow = jnp.where(level < depth, flow, 0.0)
        value = jnp.concatenate([flow, flow], axis=0).astype(jnp.bfloat16)
        left = high_rows(klass >> 3, value)
        right = low_rows(base + (klass & 7))
        for lane in range(0, cols, LANES):
            lefts.append(left[:, lane:lane + LANES])
            rights.append(right[:, lane:lane + LANES])
            if len(lefts) == 2:
                mxu, stage = count % 2, (count // 2) % 2
                count += 1
                pltpu.matmul_push_rhs(
                    jnp.concatenate(rights, axis=1), staging_register=stage, mxu_index=mxu, transpose=True)
                pltpu.matmul_acc_lhs(accs[mxu], jnp.concatenate(lefts, axis=1), load_staged_rhs=stage)
                lefts, rights = [], []


def drain(accs):
    return squeeze_rows(pltpu.matmul_pop(accs[0]) + pltpu.matmul_pop(accs[1]))


def fused_body(lats, lons, flow_ref, class_ref, basin_ref, depth_ref, sums_ref, out_ref,
               flows, classes, basins, depths, sums, table, arrived, mine, in_sems, sum_sem,
               move_send, move_recv, keep_sem, own_send, lat_send, out_recv, a0, a1, b0, b1, c0, c1):
    lat, lon = lax.axis_index("lat"), lax.axis_index("lon")
    steps = classes.shape[0]
    units = steps * (UNIT // SUB)
    column = [(lat, lax.rem(lon + k, lons)) for k in range(1, lons)]
    lat_peers = [(lax.rem(lat + k, lats), lon) for k in range(1, lats)]

    def fetch(t):
        rows = pl.ds(pl.multiple_of(t * UNIT, UNIT), UNIT)
        return [
            pltpu.make_async_copy(flow_ref.at[:, rows, :], flows.at[t], in_sems.at[0, t]),
            pltpu.make_async_copy(class_ref.at[:, rows, :], classes.at[t], in_sems.at[1, t]),
            pltpu.make_async_copy(basin_ref.at[rows, :], basins.at[t], in_sems.at[2, t]),
            pltpu.make_async_copy(depth_ref.at[rows, :], depths.at[t], in_sems.at[3, t]),
        ]

    for t in range(steps):
        for copy in fetch(t):
            copy.start()
    load = pltpu.make_async_copy(sums_ref, sums, sum_sem)
    load.start()
    barrier = pltpu.get_barrier_semaphore()
    for peer in column + lat_peers:
        pl.semaphore_signal(barrier, inc=1, device_id=peer, device_id_type=MESH)

    def remote(src, dst, send_sem, recv_sem, peer):
        return pltpu.make_async_remote_copy(
            src_ref=src, dst_ref=dst, send_sem=send_sem, recv_sem=recv_sem,
            device_id=peer, device_id_type=MESH,
        )

    def owner(u):
        zs = lons // 2
        back = lax.rem(2 * units - 1 - u, lons)
        i = lax.rem(back, zs)
        z = zs // 2 - 1 - i // 2 + lax.rem(i, 2) * (1 + 2 * (i // 2))
        return 2 * z + lax.rem(1 + back + back // zs, 2)

    def move_copy(u, k):
        return remote(table.at[u + 1], arrived.at[u, k - 1], move_send.at[u], move_recv.at[u, k - 1], (lat, owner(u)))

    def block_copy(group, u, n, peer):
        ref = out_ref.at[group * units + u]
        return remote(ref, ref, lat_send.at[u, n], out_recv.at[group * units + u], peer)

    def own_copy(u, send_sem, peer):
        return remote(mine.at[u], out_ref.at[lat * units + u], send_sem, out_recv.at[lat * units + u], peer)

    def keep_copy(u):
        return pltpu.make_async_copy(mine.at[u], out_ref.at[lat * units + u], keep_sem.at[u])

    def move(u):
        @pl.when(owner(u) != lon)
        def _():
            move_copy(u, lax.rem(lon - owner(u) + lons, lons)).start()

    def finish(u):
        @pl.when(owner(u) == lon)
        def _():
            for k in range(1, lons):
                move_copy(u, k).wait_recv()
            share = table[u + 1]
            for k in range(1, lons):
                share = share + arrived[u, k - 1]
            mine[u] = accumulate(share, sums[...], c0, c1).astype(jnp.bfloat16)
            for n, peer in enumerate(column):
                own_copy(u, own_send.at[u, n], peer).start()
            for n, peer in enumerate(lat_peers):
                own_copy(u, lat_send.at[u, n], peer).start()
            keep_copy(u).start()

    def forward(u):
        @pl.when(owner(u) != lon)
        def _():
            block_copy(lat, u, 0, column[0]).wait_recv()
            for n, peer in enumerate(lat_peers):
                block_copy(lat, u, n, peer).start()

    def from_zero(stage, u):
        @pl.when(u >= 0)
        def _():
            stage(u)

    def bin_step(t, moves):
        pairs = STEP // UNIT
        for i in range(STEP // SUB):
            n = t * pairs + i // 2
            if i == 0:
                for m in range(pairs if moves else 1):
                    for copy in fetch(n + m):
                        copy.wait()
            elif i % 2 == 0 and not moves:
                for copy in fetch(n):
                    copy.wait()
            u = t * (STEP // SUB) + i
            accs, others = ((a0, a1), (b0, b1)) if i % 2 == 0 else ((b0, b1), (a0, a1))
            table[u] = drain(others)
            refs = [flows.at[n], classes.at[n], basins.at[n], depths.at[n]]
            bin_half(*refs, i % 2, accs, (lambda u=u: move(u - 1)) if moves else None)

    per = STEP // SUB

    def step(t, carry):
        bin_step(t, True)
        for late in range(per, 0, -1):
            finish(per * t - late)
        for late in range(2 * per, per, -1):
            from_zero(forward, per * t - late)
        return carry

    bin_step(0, False)
    pl.semaphore_wait(barrier, len(column) + len(lat_peers))
    load.wait()
    for u in range(per - 1):
        move(u)
    lax.fori_loop(1, units // per, step, 0)
    table[units] = drain((b0, b1))
    last = units - 1
    move(last)
    finish(last - 3)
    finish(last - 2)
    for u in range(last - 7, last - 3):
        forward(u)
    finish(last - 1)
    forward(last - 3)
    finish(last)
    for u in range(last - 2, last + 1):
        forward(u)

    def settle(u, carry):
        for k in range(1, lats):
            block_copy(lax.rem(lat + k, lats), u, 0, column[0]).wait_recv()

        @pl.when(owner(u) == lon)
        def _():
            for n, peer in enumerate(column):
                own_copy(u, own_send.at[u, n], peer).wait_send()
            keep_copy(u).wait()

        @pl.when(owner(u) != lon)
        def _():
            move_copy(u, 1).wait_send()

        for n, peer in enumerate(lat_peers):
            block_copy(lat, u, n, peer).wait_send()
        return carry

    lax.fori_loop(0, units, settle, 0)


def fused_kernel(lats, lons, *refs):
    shape = (HIGHS * SUB, TILE)
    tail = (6 * SUB, TILE)
    pl.run_scoped(
        functools.partial(fused_body, lats, lons, *refs),
        *[pltpu.ACC(m)(s, jnp.float32) for s in (shape, shape, tail) for m in (0, 1)],
    )


def fused(lats, lons, transport, sigma_class, basin_id, depth_levels):
    levels, row_count, cols = sigma_class.shape
    steps = row_count // UNIT
    units = row_count // SUB
    width = HIGH_BLOCKS * TILE
    dma = pltpu.SemaphoreType.DMA
    hbm = pl.BlockSpec(memory_space=pltpu.HBM)
    operands = (transport, sigma_class, basin_id, depth_levels, jnp.asarray(running_sums()))
    return pl.pallas_call(
        functools.partial(fused_kernel, lats, lons),
        out_shape=jax.ShapeDtypeStruct((lats * units, SUB, width), jnp.bfloat16),
        in_specs=[hbm] * 5,
        out_specs=pl.BlockSpec(memory_space=pl.ANY),
        scratch_shapes=[
            pltpu.VMEM((steps, levels, UNIT, cols), jnp.bfloat16),
            pltpu.VMEM((steps, levels, UNIT, cols), jnp.int32),
            pltpu.VMEM((steps, UNIT, cols), jnp.int32),
            pltpu.VMEM((steps, UNIT, cols), jnp.int32),
            pltpu.VMEM((HIGH_BLOCKS * LANES, 2 * TILE), ONE_HOT),
            pltpu.VMEM((units + 1, SUB, width), jnp.float32),
            pltpu.VMEM((units, lons - 1, SUB, width), jnp.float32),
            pltpu.VMEM((units, SUB, width), jnp.bfloat16),
            dma((4, steps)), dma(()),
            dma((units,)), dma((units, lons - 1)), dma((units,)),
            dma((units, lons - 1)), dma((units, lats - 1)), dma((lats * units,)),
        ],
        compiler_params=pltpu.CompilerParams(
            collective_id=0, has_side_effects=True, vmem_limit_bytes=40 * 1024 * 1024),
        name="fused_rows",
    )(*[pltpu.with_memory_space_constraint(x, pltpu.HBM) for x in operands])


def turn_kernel(in_ref, out_ref, turned, sems):
    blocks, rows, _ = in_ref.shape
    copies = []
    for basin in range(BASINS):
        for lane in range(0, blocks * rows, LANES):
            block = in_ref[lane // rows:(lane + LANES) // rows, :, basin * TILE:(basin + 1) * TILE]
            turned[basin, :, lane:lane + LANES] = jnp.transpose(block.reshape(LANES, TILE))[:CLASSES]
        copies.append(pltpu.make_async_copy(turned.at[basin], out_ref.at[basin], sems.at[basin]))
        copies[-1].start()
    for copy in copies:
        copy.wait()


def turn(whole):
    blocks, rows, width = whole.shape
    shape = (BASINS, CLASSES, blocks * rows)
    return pl.pallas_call(
        turn_kernel,
        in_specs=[pl.BlockSpec(memory_space=pltpu.VMEM)],
        out_specs=pl.BlockSpec(memory_space=pl.ANY),
        out_shape=jax.ShapeDtypeStruct(shape, jnp.bfloat16),
        scratch_shapes=[pltpu.VMEM(shape, jnp.bfloat16), pltpu.SemaphoreType.DMA((BASINS,))],
        compiler_params=pltpu.CompilerParams(vmem_limit_bytes=16 * 1024 * 1024),
        name="turn_rows",
    )(whole)


def body(lats, lons, transport, sigma_class, basin_id, depth_levels):
    return turn(fused(lats, lons, transport, sigma_class, basin_id, depth_levels))


def solution(mesh):
    placed = (P(None, "lat", "lon"), P(None, "lat", "lon"), P("lat", "lon"), P("lat", "lon"))
    local = functools.partial(body, mesh.shape["lat"], mesh.shape["lon"])
    return jax.shard_map(local, mesh=mesh, in_specs=placed, out_specs=P(), check_vma=False)
```
